32 devices in a mesh: rep: 4 (over x, core), tp: 8 (over z, y).
Axes of the slice: x: 2, y: 2, z: 4, core: 2. Of those that a mesh axis runs over, the one named last changes fastest.
Arguments:
- trainer_query: float32 [32, 256, 8192], P(('rep', 'tp')), may hold values from -6 to 6
- trainer_output: float32 [32, 8192, 256], P(('rep', 'tp')), may hold values from -6 to 6
- probes: bfloat16 [768, 8192], replicated, may hold values from -0.0625 to 0.0625
- shard_block: int32 [32], replicated, may hold values from 0 to 31, each once
- slice_owner: int32 [8], replicated, may hold values from 0 to 7, each once
Outputs:
- query_slices: bfloat16 [8, 8192, 1024], P('tp')
- output_slices: bfloat16 [8, 1024, 8192], P('tp')
- query_prints: float32 [8, 768, 1024], P('tp')
- output_prints: float32 [8, 1024, 768], P('tp')
The draws below stay inside these ranges and needn't reach their ends.
Inputs may be any that keep to these rules, and one draw needn't show every extreme that they name: `shard_block`: a permutation: each number once. `slice_owner`: a permutation: each number once.
All inputs are finite; a program needn't handle non-finite values.
Results may differ from the reference program's by a relative error of at most 0.0029.
Values may be sent and summed in bfloat16 or wider, within the bound.
A program may use at most 192 MiB of HBM per device.

```python
import jax
import jax.numpy as jnp

D = 8192
PROBES = 768
HQ = 8192
SHARD = 256
SLICE = 1024
N_TP = 8
DEVICES = 32


def shard_levels(rng, extent, shards, low, high):
    loudness = 1.0
    for dim, blocks in shards:
        heights = jax.random.uniform(jax.random.fold_in(jax.random.fold_in(rng, 6), dim), (blocks,), jnp.float32, low / len(shards), high / len(shards))
        loudness = loudness * jnp.repeat(jnp.exp(heights), extent[dim] // blocks).reshape((-1,) + (1,) * (len(extent) - 1 - dim))
    return loudness


def noise(stream_key, shape, deviation, reach, shards=(), kind=jnp.bfloat16):
    entries = deviation * jax.random.normal(stream_key, shape, jnp.float32)
    if shards:
        entries = entries * shard_levels(stream_key, shape, shards, -0.22, 0.18)
    return jnp.clip(entries, -reach, reach).astype(kind)


def setup_inputs(seed: int = 0) -> dict:
    streams_of = jax.random.split(jax.random.key(seed), 6)
    return {
        "trainer_query": noise(streams_of[0], (DEVICES, SHARD, HQ), 1.0, 6.0, ((0, 32),), jnp.float32),
        "trainer_output": noise(streams_of[1], (DEVICES, HQ, SHARD), 1.0, 6.0, ((0, 32),), jnp.float32),
        "probes": noise(streams_of[2], (PROBES, D), D ** -0.5, 0.0625),
        "shard_block": jax.random.permutation(streams_of[3], DEVICES).astype(jnp.int32),
        "slice_owner": jax.random.permutation(streams_of[4], N_TP).astype(jnp.int32),
    }


def reference(trainer_query, trainer_output, probes, shard_block, slice_owner):
    positions = jnp.arange(DEVICES, dtype=jnp.int32)
    inverse = jnp.zeros((DEVICES,), jnp.int32).at[shard_block].set(positions)
    query_full = trainer_query.astype(jnp.bfloat16)[inverse].reshape(D, HQ)
    output_full = jnp.transpose(trainer_output.astype(jnp.bfloat16)[inverse], (1, 0, 2)).reshape(HQ, D)
    query_slices = jnp.transpose(query_full.reshape(D, N_TP, SLICE)[:, slice_owner], (1, 0, 2))
    output_slices = output_full.reshape(N_TP, SLICE, D)[slice_owner]
    probe_wide = probes.astype(jnp.float32)
    query_prints = jnp.einsum("pd,jdc->jpc", probe_wide, query_slices.astype(jnp.float32))
    output_prints = jnp.einsum("jcd,pd->jcp", output_slices.astype(jnp.float32), probe_wide)
    return (query_slices, output_slices, query_prints, output_prints)
```

```python
import functools

import jax
import jax.numpy as jnp
from jax import lax
from jax.experimental import pallas as pl
from jax.experimental.pallas import tpu as pltpu
from jax.sharding import PartitionSpec as P

MESH = pl.DeviceIdType.MESH
VMEM_LIMIT = 99 * 256 * 1024


def pack_kernel(owner_ref, query_ref, output_ref, query_blocks, output_blocks):
    query_blocks[...] = query_ref[...].astype(jnp.bfloat16)
    output_blocks[...] = output_ref[...].astype(jnp.bfloat16)


def pack(trainer_query, trainer_output, slice_owner):
    tp_count = slice_owner.shape[0]
    _, rows, width = trainer_query.shape
    cut = width // tp_count
    return pl.pallas_call(
        pack_kernel,
        out_shape=(
            jax.ShapeDtypeStruct((tp_count, rows, cut), jnp.bfloat16),
            jax.ShapeDtypeStruct((tp_count, cut, rows), jnp.bfloat16),
        ),
        grid_spec=pltpu.PrefetchScalarGridSpec(
            num_scalar_prefetch=1,
            grid=(tp_count,),
            in_specs=[
                pl.BlockSpec((1, rows, cut), lambda k, owner: (0, 0, owner[k])),
                pl.BlockSpec((1, cut, rows), lambda k, owner: (0, owner[k], 0)),
            ],
            out_specs=[
                pl.BlockSpec((1, rows, cut), lambda k, owner: (k, 0, 0)),
                pl.BlockSpec((1, cut, rows), lambda k, owner: (k, 0, 0)),
            ],
        ),
    )(slice_owner, trainer_query, trainer_output)


def pair_index(index, offset, count):
    paired, bit = 0, 1
    while bit < count:
        low = lax.rem(lax.div(index, bit) + lax.div(offset, bit), 2)
        paired = paired + bit * low
        bit *= 2
    return paired


def move_kernel(rep_count, tp_count, multiply, *refs):
    if multiply:
        (owner_ref, query_blocks, output_blocks, probes_ref,
         query_all, output_all, query_prints, output_prints,
         swap_send, swap_recv, near_send, near_recv, far_send, far_recv, own_sem,
         probes, picked, query_tile, output_tile, load_sem, probes_sem) = refs
    else:
        (query_blocks, output_blocks, query_all, output_all,
         swap_send, swap_recv, near_send, near_recv, far_send, far_recv, own_sem) = refs
    rep, tp = lax.axis_index("rep"), lax.axis_index("tp")
    partner = rep + 1 - 2 * lax.rem(rep, 2)
    hops = range(1, rep_count // 2)
    ahead = {hop: lax.rem(rep + 2 * hop, rep_count) for hop in hops}
    behind = {hop: lax.rem(rep + rep_count - 2 * hop, rep_count) for hop in hops}
    across = {hop: lax.rem(partner + rep_count - 2 * hop, rep_count) for hop in hops}
    arrays = ((query_blocks, query_all), (output_blocks, output_all))
    mine = rep * tp_count + tp
    count = rep_count * tp_count
    rows = query_blocks.shape[1]

    def load_probes(block):
        columns = pl.ds(pl.multiple_of(block * rows, rows), rows)
        return pltpu.make_async_copy(
            probes_ref.at[:, columns], probes.at[block], probes_sem.at[block]
        )

    def pair(offset):
        return pair_index(tp, jnp.int32(offset), tp_count)

    barrier = pltpu.get_barrier_semaphore()
    peers = [(rep, pair(offset)) for offset in range(1, tp_count)]
    peers += [(partner, tp)] + [(ahead[hop], tp) for hop in hops]
    for peer in peers:
        pl.semaphore_signal(barrier, inc=1, device_id=peer, device_id_type=MESH)
    pl.semaphore_wait(barrier, len(peers))

    def remote(source, target, send_sem, recv_sem, device):
        return pltpu.make_async_remote_copy(
            src_ref=source, dst_ref=target, send_sem=send_sem, recv_sem=recv_sem,
            device_id=device, device_id_type=MESH,
        )

    def swap(offset, a):
        blocks, everything = arrays[a]
        return remote(
            blocks.at[pair(offset)], everything.at[mine],
            swap_send.at[a, offset], swap_recv.at[a, offset], (rep, pair(offset)),
        )

    def far(hop, offset, a, block, place):
        return remote(
            block, place, far_send.at[hop - 1, a, offset], far_recv.at[hop - 1, a, offset],
            (ahead[hop], tp),
        )

    def near(hop, offset, a, block, place):
        return remote(
            block, place, near_send.at[hop, a, offset], near_recv.at[hop, a, offset],
            (partner, tp),
        )

    def place_of(group, offset, a):
        return arrays[a][1].at[group * tp_count + pair(offset)]

    def own(a):
        blocks, everything = arrays[a]
        return pltpu.make_async_copy(blocks.at[tp], everything.at[mine], own_sem.at[a])

    def spread(offset, a, block):
        place = place_of(rep, offset, a)
        for hop in hops:
            far(hop, offset, a, block, place).start()
        near(0, offset, a, block, place).start()

    def relay(offset, a):
        for hop in hops:
            place = place_of(behind[hop], offset, a)
            far(hop, offset, a, place, place).wait_recv()
            near(hop, offset, a, place, place).start()

    def collect(offset, a):
        for hop in (0, *hops):
            place = place_of(rep, offset, a)
            near(hop, offset, a, place, place).wait_recv()

        @pl.when(offset == 0)
        def _():
            own(a).wait()
            if multiply and a == 0:

                @pl.loop(0, count)
                def _(block):
                    load_probes(block).wait()


        if not multiply:
            return
        groups = [rep, partner]
        for hop in hops:
            groups += [behind[hop], across[hop]]
        tile, prints = ((query_tile, query_prints), (output_tile, output_prints))[a]
        loads = []
        for j, group in enumerate(groups):
            spot = (pl.ds(j * rows, rows), slice(None))
            load = pltpu.make_async_copy(
                place_of(group, offset, a), tile.at[spot if a == 0 else spot[::-1]],
                load_sem.at[a, j],
            )
            load.start()
            loads.append(load)
        for j, group in enumerate(groups):
            owner = owner_ref[group * tp_count + pair(offset)]
            picked[:, j * rows : (j + 1) * rows] = probes[owner]
        for load in loads:
            load.wait()
        if a == 0:
            prints[0] += jnp.dot(picked[...], tile[...], preferred_element_type=jnp.float32)
        else:
            prints[0] += lax.dot_general(
                tile[...], picked[...], (((1,), (1,)), ((), ())),
                preferred_element_type=jnp.float32,
            )

    for offset in range(1, tp_count):
        for a in range(2):
            swap(offset, a).start()
    for a in range(2):
        spread(jnp.int32(0), a, arrays[a][0].at[tp])
    for a in range(2):
        own(a).start()
    if multiply:

        @pl.loop(0, count)
        def _(block):
            load_probes(block).start()

        query_prints[...] = jnp.zeros_like(query_prints)
        output_prints[...] = jnp.zeros_like(output_prints)

    @pl.loop(1, tp_count + 2)
    def _(step):
        for a in range(2):

            @pl.when(step < tp_count)
            def _():
                swap(step, a).wait_recv()
                spread(step, a, place_of(rep, step, a))

            @pl.when(step <= tp_count)
            def _():
                relay(step - 1, a)

            if a == 0:

                @pl.when(step >= 2)
                def _():
                    collect(step - 2, 1)

            else:

                @pl.when(step <= tp_count)
                def _():
                    collect(step - 1, 0)

    @pl.loop(0, tp_count)
    def _(offset):
        for a in range(2):

            @pl.when(offset > 0)
            def _():
                swap(offset, a).wait_send()

            place = place_of(rep, offset, a)
            for hop in hops:
                far(hop, offset, a, place, place).wait_send()
            for hop in (0, *hops):
                near(hop, offset, a, place, place).wait_send()


def move(query_blocks, output_blocks, probes, shard_block, rep_count, multiply):
    tp_count, rows, cut = query_blocks.shape
    count = rep_count * tp_count
    half = rep_count // 2
    kinds = probes.shape[0]
    dma = pltpu.SemaphoreType.DMA
    anywhere = pl.BlockSpec(memory_space=pl.ANY)
    shapes = [
        jax.ShapeDtypeStruct((count, rows, cut), jnp.bfloat16),
        jax.ShapeDtypeStruct((count, cut, rows), jnp.bfloat16),
    ]
    scratch = [
        dma((2, tp_count)), dma((2, tp_count)),
        dma((half, 2, tp_count)), dma((half, 2, tp_count)),
        dma((half - 1, 2, tp_count)), dma((half - 1, 2, tp_count)),
        dma((2,)),
    ]
    operands, in_specs, out_specs = [query_blocks, output_blocks], [anywhere] * 2, [anywhere] * 2
    if multiply:
        operands = [shard_block] + operands + [probes]
        in_specs = [pl.BlockSpec(memory_space=pltpu.SMEM)] + [anywhere] * 3
        out_specs += [pl.BlockSpec(memory_space=pltpu.VMEM)] * 2
        shapes += [
            jax.ShapeDtypeStruct((1, kinds, cut), jnp.float32),
            jax.ShapeDtypeStruct((1, cut, kinds), jnp.float32),
        ]
        scratch += [
            pltpu.VMEM((count, kinds, rows), jnp.bfloat16),
            pltpu.VMEM((kinds, rep_count * rows), jnp.bfloat16),
            pltpu.VMEM((rep_count * rows, cut), jnp.bfloat16),
            pltpu.VMEM((cut, rep_count * rows), jnp.bfloat16),
            dma((2, rep_count)),
            dma((count,)),
        ]
    return pl.pallas_call(
        functools.partial(move_kernel, rep_count, tp_count, multiply),
        out_shape=shapes,
        in_specs=in_specs,
        out_specs=out_specs,
        scratch_shapes=scratch,
        compiler_params=pltpu.CompilerParams(collective_id=0, has_side_effects=True),
    )(*operands)


def order_kernel(group, inverse_ref, *refs):
    queries, outputs = refs[:group], refs[group : 2 * group]
    query_slice, output_slice = refs[2 * group :]
    rows = queries[0].shape[1]
    for j in range(group):
        query_slice[0, j * rows : (j + 1) * rows, :] = queries[j][0]
        output_slice[0, :, j * rows : (j + 1) * rows] = outputs[j][0]


def order(query_all, output_all, inverse):
    count, rows, cut = query_all.shape
    group = max(1, min(count, 1024 // rows))
    picks = range(group)
    return pl.pallas_call(
        functools.partial(order_kernel, group),
        out_shape=(
            jax.ShapeDtypeStruct((1, count * rows, cut), jnp.bfloat16),
            jax.ShapeDtypeStruct((1, cut, count * rows), jnp.bfloat16),
        ),
        grid_spec=pltpu.PrefetchScalarGridSpec(
            num_scalar_prefetch=1,
            grid=(count // group,),
            in_specs=[
                pl.BlockSpec((1, rows, cut), lambda b, inv, j=j: (inv[b * group + j], 0, 0))
                for j in picks
            ]
            + [
                pl.BlockSpec((1, cut, rows), lambda b, inv, j=j: (inv[b * group + j], 0, 0))
                for j in picks
            ],
            out_specs=[
                pl.BlockSpec((1, group * rows, cut), lambda b, inv: (0, b, 0)),
                pl.BlockSpec((1, cut, group * rows), lambda b, inv: (0, 0, b)),
            ],
        ),
    )(inverse, *([query_all] * group), *([output_all] * group))


def query_kernel(group, inverse_ref, *refs):
    blocks, (probes_ref, slice_ref, prints_ref) = refs[:group], refs[group:]
    rows = blocks[0].shape[1]
    for j, block in enumerate(blocks):
        slice_ref[0, j * rows : (j + 1) * rows, :] = block[0]
    part = jnp.dot(probes_ref[...], slice_ref[0], preferred_element_type=jnp.float32)

    @pl.when(pl.program_id(0) == 0)
    def _():
        prints_ref[0] = part

    @pl.when(pl.program_id(0) > 0)
    def _():
        prints_ref[0] += part


def output_kernel(group, inverse_ref, *refs):
    blocks, (probes_ref, slice_ref, prints_ref) = refs[:group], refs[group:]
    rows = blocks[0].shape[2]
    for j, block in enumerate(blocks):
        slice_ref[0, :, j * rows : (j + 1) * rows] = block[0]
    part = lax.dot_general(
        slice_ref[0], probes_ref[...], (((1,), (1,)), ((), ())),
        preferred_element_type=jnp.float32,
    )

    @pl.when(pl.program_id(0) == 0)
    def _():
        prints_ref[0] = part

    @pl.when(pl.program_id(0) > 0)
    def _():
        prints_ref[0] += part


def finish(body, everything, probes, inverse, slice_shape, prints_shape, along):
    count = everything.shape[0]
    block = everything.shape[1:]
    group = max(1, min(count, 1024 // block[along]))
    span = group * block[along]
    tile = list((1,) + block)
    tile[1 + along] = span
    in_specs = [
        pl.BlockSpec((1,) + block, lambda b, inv, j=j: (inv[b * group + j], 0, 0))
        for j in range(group)
    ]
    in_specs.append(pl.BlockSpec((probes.shape[0], span), lambda b, inv: (0, b)))
    place = (lambda b, inv: (0, b, 0)) if along == 0 else (lambda b, inv: (0, 0, b))
    return pl.pallas_call(
        functools.partial(body, group),
        out_shape=(
            jax.ShapeDtypeStruct(slice_shape, jnp.bfloat16),
            jax.ShapeDtypeStruct(prints_shape, jnp.float32),
        ),
        grid_spec=pltpu.PrefetchScalarGridSpec(
            num_scalar_prefetch=1,
            grid=(count // group,),
            in_specs=in_specs,
            out_specs=[
                pl.BlockSpec(tuple(tile), place),
                pl.BlockSpec(prints_shape, lambda b, inv: (0, 0, 0)),
            ],
        ),
    )(inverse, *([everything] * group), probes)


def stream_kernel(shard_ref, owner_ref, query_ref, output_ref, probes_ref,
                  query_all, output_all, query_prints, output_prints,
                  stage_even, stage_odd, query_out, output_out, probes, picked, query_tile, output_tile,
                  stage_sem, probes_sem, swap_send, swap_recv, far_send, far_recv,
                  near_send, near_recv):
    rep_count, tp_count = lax.axis_size("rep"), lax.axis_size("tp")
    rep, tp = lax.axis_index("rep"), lax.axis_index("tp")
    count, rows, cut = query_all.shape
    half = tp_count // 2
    parts = cut // stage_even.shape[2]
    size = stage_even.shape[2]
    partner = rep + 1 - 2 * lax.rem(rep, 2)
    facing = lax.rem(rep + 2, rep_count)
    behind = facing + 1 - 2 * lax.rem(facing, 2)
    mine = rep * tp_count + tp
    inner = lax.rem(lax.div(lax.div(tp, 2) + 1, 2), 2)
    everything = (query_all, output_all)
    stage = (stage_even, stage_odd)
    outgoing = (query_out, output_out)
    ticks = half * parts

    def pair(offset):
        return pair_index(tp, jnp.int32(offset), tp_count)

    def spot(a, part):
        piece = pl.ds(pl.multiple_of(part * size, size), size)
        return (slice(None), piece) if a == 0 else (piece, slice(None))

    def remote(source, target, send_sem, recv_sem, device):
        return pltpu.make_async_remote_copy(
            src_ref=source, dst_ref=target, send_sem=send_sem, recv_sem=recv_sem,
            device_id=device, device_id_type=MESH,
        )

    def swap(a, offset, part):
        return remote(
            outgoing[a].at[(offset - 1, *spot(a, part))],
            everything[a].at[(mine, *spot(a, part))],
            swap_send.at[a], swap_recv.at[a, offset, part], (rep, pair(offset)),
        )

    def held(group, a, offset, part):
        return everything[a].at[(group * tp_count + pair(offset), *spot(a, part))]

    def far(a, offset, part):
        place = held(rep, a, offset, part)
        return remote(place, place, far_send.at[a], far_recv.at[a, offset, part], (facing, tp))

    def near(kind, a, offset, part):
        place = held((rep, facing)[kind], a, offset, part)
        return remote(
            place, place, near_send.at[kind, a], near_recv.at[kind, a, offset, part],
            (partner, tp),
        )

    def load(a, part, h):
        copies = []
        depth = size // 2
        for k in range(tp_count):
            if a == 0:
                piece = pl.ds(pl.multiple_of(k * cut + part * size, size), size)
                source = query_ref.at[0, h * rows // 2 : (h + 1) * rows // 2, piece]
            else:
                piece = pl.ds(pl.multiple_of(k * cut + part * size + h * depth, depth), depth)
                source = output_ref.at[0, piece, :]
            copies.append(pltpu.make_async_copy(source, stage[h].at[k], stage_sem.at[h, k]))
        return copies

    def start_load(a, part, h):
        for copy in load(a, part, h):
            copy.start()

    def convert(part):
        for a in range(2):
            for h in range(2):
                for copy in load(a, part, h):
                    copy.wait()
                if a == 0:
                    piece = pl.ds(pl.multiple_of(part * size, size), size)
                    where = (slice(h * rows // 2, (h + 1) * rows // 2), piece)
                else:
                    depth = size // 2
                    piece = pl.ds(pl.multiple_of(part * size + h * depth, depth), depth)
                    where = (piece, slice(None))
                everything[a][(mine, *where)] = stage[h][owner_ref[tp]].astype(jnp.bfloat16)

                @pl.loop(1, tp_count)
                def _(offset):
                    outgoing[a][(offset - 1, *where)] = stage[h][
                        owner_ref[pair(offset)]
                    ].astype(jnp.bfloat16)

                if a == 0:
                    start_load(1, part, h)
                else:

                    @pl.when(part < parts - 1)
                    def _():
                        start_load(0, part + 1, h)

    def far_offset(e):
        return half + 2 * lax.rem(lax.div(e, 2) + inner, 2) + lax.rem(e, 2)

    def spread(a, offset, part):
        far(a, offset, part).start()
        near(0, a, offset, part).start()

    def send_near(part):
        @pl.loop(1, half)
        def _(offset):
            for a in range(2):
                swap(a, offset, part).start()

    def send_far(part):
        @pl.loop(0, half)
        def _(e):
            for a in range(2):
                swap(a, far_offset(e), part).start()

    def item(p):
        late = lax.div(p, 2 * ticks - half)
        begun = lax.div(p + 2 * ticks - half, 2 * ticks)
        mm = lax.div(p + half, 2) - half
        b = lax.rem(p, 2)
        is_far = begun * ((1 - late) * (1 - b) + late)
        fm = late * (p - ticks) + (1 - late) * mm
        fm = fm * is_far
        near_part = begun * lax.div(mm + half, half)
        near_offset = (1 - begun) * p + begun * lax.rem(mm + half, half)
        offset = is_far * far_offset(lax.rem(fm, half)) + (1 - is_far) * near_offset
        part = is_far * lax.div(fm, half) + (1 - is_far) * near_part
        return offset, part

    def relay(p):
        offset, part = item(p)
        for a in range(2):
            far(a, offset, part).wait_recv()
            near(1, a, offset, part).start()

    def collect(p):
        offset, part = item(p)
        groups = (rep, partner, facing, behind)
        for a in range(2):
            for kind in range(2):
                near(kind, a, offset, part).wait_recv()
        for g, group in enumerate(groups):
            source = group * tp_count + pair(offset)
            strip = slice(g * rows, (g + 1) * rows)
            picked[:, strip] = probes[shard_ref[source]]
            query_tile[strip, :] = query_all[(source, *spot(0, part))]
            output_tile[:, strip] = output_all[(source, *spot(1, part))]
        query_prints[(0, *spot(0, part))] += jnp.dot(
            picked[...], query_tile[...], preferred_element_type=jnp.float32
        )
        output_prints[(0, *spot(1, part))] += lax.dot_general(
            output_tile[...], picked[...], (((1,), (1,)), ((), ())),
            preferred_element_type=jnp.float32,
        )

    def load_probes(block):
        columns = pl.ds(pl.multiple_of(block * rows, rows), rows)
        return pltpu.make_async_copy(
            probes_ref.at[:, columns], probes.at[block], probes_sem.at[block]
        )

    for h in range(2):
        start_load(0, 0, h)
    barrier = pltpu.get_barrier_semaphore()
    peers = [(rep, pair(offset)) for offset in range(1, tp_count)]
    peers += [(partner, tp), (facing, tp)]
    for peer in peers:
        pl.semaphore_signal(barrier, inc=1, device_id=peer, device_id_type=MESH)
    convert(jnp.int32(0))
    pl.semaphore_wait(barrier, len(peers))

    for a in range(2):
        spread(a, jnp.int32(0), 0)

    @pl.when(inner == 1)
    def _():
        send_far(0)

    send_near(0)
    convert(jnp.int32(1))
    send_near(1)

    @pl.when(inner == 0)
    def _():
        send_far(0)

    @pl.loop(0, count)
    def _(block):
        load_probes(block).start()

    query_prints[...] = jnp.zeros_like(query_prints)
    output_prints[...] = jnp.zeros_like(output_prints)

    @pl.loop(1, half)
    def _(offset):
        for a in range(2):
            swap(a, offset, 0).wait_recv()
            spread(a, offset, 0)

    @pl.loop(0, count)
    def _(block):
        load_probes(block).wait()

    @pl.loop(0, ticks + 2)
    def _(m):
        @pl.loop(0, 2)
        def _(i):
            p = 2 * m - 3 + i

            @pl.when((p >= 0) & (p < 2 * ticks))
            def _():
                collect(p)

        q = lax.div(m, half)
        j = lax.rem(m, half)

        @pl.when(m < ticks)
        def _():
            offset = far_offset(j)
            for a in range(2):
                swap(a, offset, q).wait_recv()
                spread(a, offset, q)

        @pl.when(m < ticks - half)
        def _():
            @pl.when(j > 0)
            def _():
                for a in range(2):
                    swap(a, j, q + 1).wait_recv()

            for a in range(2):
                spread(a, j, q + 1)

            @pl.when((j == 1) & (q < parts - 2))
            def _():
                convert(q + 2)

            @pl.when(j == 2)
            def _():
                @pl.when(inner == 1)
                def _():
                    send_far(q + 1)

                @pl.when(q < parts - 2)
                def _():
                    send_near(q + 2)

                @pl.when(inner == 0)
                def _():
                    send_far(q + 1)

        @pl.loop(0, 2)
        def _(i):
            p = 2 * m - 1 + i

            @pl.when((p >= 0) & (p < 2 * ticks))
            def _():
                relay(p)

    for a in range(2):
        whole = outgoing[a]
        remote(whole, whole, swap_send.at[a], swap_recv.at[a, 0, 0], (partner, tp)).wait_send()
        whole = everything[a].at[pl.ds(0, tp_count)]
        for sem in (far_send.at[a], near_send.at[0, a], near_send.at[1, a]):
            remote(whole, whole, sem, swap_recv.at[a, 0, 0], (partner, tp)).wait_send()


def stream(trainer_query, trainer_output, probes, shard_block, slice_owner, rep_count):
    tp_count = slice_owner.shape[0]
    _, rows, width = trainer_query.shape
    cut = width // tp_count
    count = rep_count * tp_count
    kinds = probes.shape[0]
    parts = 4
    size = cut // parts
    dma = pltpu.SemaphoreType.DMA
    anywhere = pl.BlockSpec(memory_space=pl.ANY)
    small = pl.BlockSpec(memory_space=pltpu.SMEM)
    depth = rep_count * rows
    return pl.pallas_call(
        stream_kernel,
        out_shape=[
            pltpu.VMEM((count, rows, cut), jnp.bfloat16),
            pltpu.VMEM((count, cut, rows), jnp.bfloat16),
            pltpu.VMEM((1, kinds, cut), jnp.float32),
            pltpu.VMEM((1, cut, kinds), jnp.float32),
        ],
        in_specs=[small, small, anywhere, anywhere, anywhere],
        out_specs=[pl.BlockSpec(memory_space=pltpu.VMEM)] * 4,
        scratch_shapes=[
            pltpu.VMEM((tp_count, size // 2, size), jnp.float32),
            pltpu.VMEM((tp_count, size // 2, size), jnp.float32),
            pltpu.VMEM((tp_count - 1, rows, cut), jnp.bfloat16),
            pltpu.VMEM((tp_count - 1, cut, rows), jnp.bfloat16),
            pltpu.VMEM((count, kinds, rows), jnp.bfloat16),
            pltpu.VMEM((kinds, depth), jnp.bfloat16),
            pltpu.VMEM((depth, size), jnp.bfloat16),
            pltpu.VMEM((size, depth), jnp.bfloat16),
            dma((2, tp_count)), dma((count,)),
            dma((2,)), dma((2, tp_count, parts)),
            dma((2,)), dma((2, tp_count, parts)),
            dma((2, 2)), dma((2, 2, tp_count, parts)),
        ],
        compiler_params=pltpu.CompilerParams(
            collective_id=0, has_side_effects=True, vmem_limit_bytes=VMEM_LIMIT
        ),
    )(shard_block, slice_owner, trainer_query, trainer_output, probes)


def place_kernel(shard_ref, query_all, output_all, query_prints, output_prints,
                 query_slice, output_slice, query_result, output_result, sems):
    count, rows, _ = query_all.shape

    @pl.loop(0, count)
    def _(source):
        block = pl.ds(pl.multiple_of(shard_ref[source] * rows, rows), rows)
        pltpu.make_async_copy(
            query_all.at[source], query_slice.at[0, block, :], sems.at[0]
        ).start()
        pltpu.make_async_copy(
            output_all.at[source], output_slice.at[0, :, block], sems.at[1]
        ).start()

    prints = (
        pltpu.make_async_copy(query_prints, query_result, sems.at[2]),
        pltpu.make_async_copy(output_prints, output_result, sems.at[3]),
    )
    for copy in prints:
        copy.start()
    for k, everything in enumerate((query_all, output_all)):
        pltpu.make_async_copy(everything, everything, sems.at[k]).wait()
    for copy in prints:
        copy.wait()


def place(moved, shard_block):
    query_all, output_all, query_prints, output_prints = moved
    count, rows, cut = query_all.shape
    inside = pl.BlockSpec(memory_space=pltpu.VMEM)
    return pl.pallas_call(
        place_kernel,
        out_shape=(
            jax.ShapeDtypeStruct((1, count * rows, cut), jnp.bfloat16),
            jax.ShapeDtypeStruct((1, cut, count * rows), jnp.bfloat16),
            jax.ShapeDtypeStruct(query_prints.shape, jnp.float32),
            jax.ShapeDtypeStruct(output_prints.shape, jnp.float32),
        ),
        in_specs=[pl.BlockSpec(memory_space=pltpu.SMEM)] + [inside] * 4,
        out_specs=[pl.BlockSpec(memory_space=pl.ANY)] * 4,
        scratch_shapes=[pltpu.SemaphoreType.DMA((4,))],
        compiler_params=pltpu.CompilerParams(vmem_limit_bytes=VMEM_LIMIT),
    )(shard_block, *(pltpu.with_memory_space_constraint(x, pltpu.VMEM) for x in moved))


def per_device(trainer_query, trainer_output, probes, shard_block, slice_owner):
    tp_count = lax.axis_size("tp")
    rep_count = lax.axis_size("rep")
    count = tp_count * rep_count
    rows, width = trainer_query.shape[1:]
    cut = width // tp_count
    model = rows * count
    if rep_count == 4 and tp_count == 8 and rows % 128 == 0 and cut == 4 * rows:
        moved = stream(
            trainer_query, trainer_output, probes, shard_block, slice_owner, rep_count
        )
        return place(moved, shard_block)
    positions = jnp.arange(count, dtype=jnp.int32)
    held = shard_block[None, :] == positions[:, None]
    inverse = jnp.sum(jnp.where(held, positions[None, :], 0), axis=1, dtype=jnp.int32)
    query_blocks, output_blocks = pack(trainer_query, trainer_output, slice_owner)
    multiply = rows % 128 == 0
    moved = move(query_blocks, output_blocks, probes, shard_block, rep_count, multiply)
    if multiply:
        query_all, output_all, query_prints, output_prints = moved
        query_slice, output_slice = order(query_all, output_all, inverse)
        return query_slice, output_slice, query_prints, output_prints
    query_all, output_all = moved
    query_slice, query_prints = finish(
        query_kernel, query_all, probes, inverse,
        (1, model, cut), (1, probes.shape[0], cut), 0,
    )
    output_slice, output_prints = finish(
        output_kernel, output_all, probes, inverse,
        (1, cut, model), (1, cut, probes.shape[0]), 1,
    )
    return query_slice, output_slice, query_prints, output_prints


def solution(mesh):
    placed = (P(("rep", "tp"), None, None), P(("rep", "tp"), None, None), P(), P(), P())
    return jax.shard_map(
        per_device,
        mesh=mesh,
        in_specs=placed,
        out_specs=(
            P("tp", None, None),
            P("tp", None, None),
            P("tp", None, None),
            P("tp", None, None),
        ),
        check_vma=False,
    )
```

```python
import functools

import jax
import jax.numpy as jnp
from jax import lax
from jax.experimental import pallas as pl
from jax.experimental.pallas import tpu as pltpu
from jax.sharding import PartitionSpec as P

MESH = pl.DeviceIdType.MESH
VMEM_LIMIT = 99 * 256 * 1024
LEAD = 3
LAG = 1


def pack_kernel(owner_ref, query_ref, output_ref, query_blocks, output_blocks):
    query_blocks[...] = query_ref[...].astype(jnp.bfloat16)
    output_blocks[...] = output_ref[...].astype(jnp.bfloat16)


def pack(trainer_query, trainer_output, slice_owner):
    tp_count = slice_owner.shape[0]
    _, rows, width = trainer_query.shape
    cut = width // tp_count
    return pl.pallas_call(
        pack_kernel,
        out_shape=(
            jax.ShapeDtypeStruct((tp_count, rows, cut), jnp.bfloat16),
            jax.ShapeDtypeStruct((tp_count, cut, rows), jnp.bfloat16),
        ),
        grid_spec=pltpu.PrefetchScalarGridSpec(
            num_scalar_prefetch=1,
            grid=(tp_count,),
            in_specs=[
                pl.BlockSpec((1, rows, cut), lambda k, owner: (0, 0, owner[k])),
                pl.BlockSpec((1, cut, rows), lambda k, owner: (0, owner[k], 0)),
            ],
            out_specs=[
                pl.BlockSpec((1, rows, cut), lambda k, owner: (k, 0, 0)),
                pl.BlockSpec((1, cut, rows), lambda k, owner: (k, 0, 0)),
            ],
        ),
    )(slice_owner, trainer_query, trainer_output)


def pair_index(index, offset, count):
    paired, bit = 0, 1
    while bit < count:
        low = lax.rem(lax.div(index, bit) + lax.div(offset, bit), 2)
        paired = paired + bit * low
        bit *= 2
    return paired


def move_kernel(rep_count, tp_count, multiply, *refs):
    if multiply:
        (owner_ref, query_blocks, output_blocks, probes_ref,
         query_all, output_all, query_prints, output_prints,
         swap_send, swap_recv, near_send, near_recv, far_send, far_recv, own_sem,
         probes, picked, query_tile, output_tile, load_sem, probes_sem) = refs
    else:
        (query_blocks, output_blocks, query_all, output_all,
         swap_send, swap_recv, near_send, near_recv, far_send, far_recv, own_sem) = refs
    rep, tp = lax.axis_index("rep"), lax.axis_index("tp")
    partner = rep + 1 - 2 * lax.rem(rep, 2)
    hops = range(1, rep_count // 2)
    ahead = {hop: lax.rem(rep + 2 * hop, rep_count) for hop in hops}
    behind = {hop: lax.rem(rep + rep_count - 2 * hop, rep_count) for hop in hops}
    across = {hop: lax.rem(partner + rep_count - 2 * hop, rep_count) for hop in hops}
    arrays = ((query_blocks, query_all), (output_blocks, output_all))
    mine = rep * tp_count + tp
    count = rep_count * tp_count
    rows = query_blocks.shape[1]

    def load_probes(block):
        columns = pl.ds(pl.multiple_of(block * rows, rows), rows)
        return pltpu.make_async_copy(
            probes_ref.at[:, columns], probes.at[block], probes_sem.at[block]
        )

    def pair(offset):
        return pair_index(tp, jnp.int32(offset), tp_count)

    barrier = pltpu.get_barrier_semaphore()
    peers = [(rep, pair(offset)) for offset in range(1, tp_count)]
    peers += [(partner, tp)] + [(ahead[hop], tp) for hop in hops]
    for peer in peers:
        pl.semaphore_signal(barrier, inc=1, device_id=peer, device_id_type=MESH)
    pl.semaphore_wait(barrier, len(peers))

    def remote(source, target, send_sem, recv_sem, device):
        return pltpu.make_async_remote_copy(
            src_ref=source, dst_ref=target, send_sem=send_sem, recv_sem=recv_sem,
            device_id=device, device_id_type=MESH,
        )

    def swap(offset, a):
        blocks, everything = arrays[a]
        return remote(
            blocks.at[pair(offset)], everything.at[mine],
            swap_send.at[a, offset], swap_recv.at[a, offset], (rep, pair(offset)),
        )

    def far(hop, offset, a, block, place):
        return remote(
            block, place, far_send.at[hop - 1, a, offset], far_recv.at[hop - 1, a, offset],
            (ahead[hop], tp),
        )

    def near(hop, offset, a, block, place):
        return remote(
            block, place, near_send.at[hop, a, offset], near_recv.at[hop, a, offset],
            (partner, tp),
        )

    def place_of(group, offset, a):
        return arrays[a][1].at[group * tp_count + pair(offset)]

    def own(a):
        blocks, everything = arrays[a]
        return pltpu.make_async_copy(blocks.at[tp], everything.at[mine], own_sem.at[a])

    def spread(offset, a, block):
        place = place_of(rep, offset, a)
        for hop in hops:
            far(hop, offset, a, block, place).start()
        near(0, offset, a, block, place).start()

    def relay(offset, a):
        for hop in hops:
            place = place_of(behind[hop], offset, a)
            far(hop, offset, a, place, place).wait_recv()
            near(hop, offset, a, place, place).start()

    def collect(offset, a):
        for hop in (0, *hops):
            place = place_of(rep, offset, a)
            near(hop, offset, a, place, place).wait_recv()

        @pl.when(offset == 0)
        def _():
            own(a).wait()
            if multiply and a == 0:

                @pl.loop(0, count)
                def _(block):
                    load_probes(block).wait()


        if not multiply:
            return
        groups = [rep, partner]
        for hop in hops:
            groups += [behind[hop], across[hop]]
        tile, prints = ((query_tile, query_prints), (output_tile, output_prints))[a]
        loads = []
        for j, group in enumerate(groups):
            spot = (pl.ds(j * rows, rows), slice(None))
            load = pltpu.make_async_copy(
                place_of(group, offset, a), tile.at[spot if a == 0 else spot[::-1]],
                load_sem.at[a, j],
            )
            load.start()
            loads.append(load)
        for j, group in enumerate(groups):
            owner = owner_ref[group * tp_count + pair(offset)]
            picked[:, j * rows : (j + 1) * rows] = probes[owner]
        for load in loads:
            load.wait()
        if a == 0:
            prints[0] += jnp.dot(picked[...], tile[...], preferred_element_type=jnp.float32)
        else:
            prints[0] += lax.dot_general(
                tile[...], picked[...], (((1,), (1,)), ((), ())),
                preferred_element_type=jnp.float32,
            )

    for offset in range(1, tp_count):
        for a in range(2):
            swap(offset, a).start()
    for a in range(2):
        spread(jnp.int32(0), a, arrays[a][0].at[tp])
    for a in range(2):
        own(a).start()
    if multiply:

        @pl.loop(0, count)
        def _(block):
            load_probes(block).start()

        query_prints[...] = jnp.zeros_like(query_prints)
        output_prints[...] = jnp.zeros_like(output_prints)

    @pl.loop(1, tp_count + 2)
    def _(step):
        for a in range(2):

            @pl.when(step < tp_count)
            def _():
                swap(step, a).wait_recv()
                spread(step, a, place_of(rep, step, a))

            @pl.when(step <= tp_count)
            def _():
                relay(step - 1, a)

            if a == 0:

                @pl.when(step >= 2)
                def _():
                    collect(step - 2, 1)

            else:

                @pl.when(step <= tp_count)
                def _():
                    collect(step - 1, 0)

    @pl.loop(0, tp_count)
    def _(offset):
        for a in range(2):

            @pl.when(offset > 0)
            def _():
                swap(offset, a).wait_send()

            place = place_of(rep, offset, a)
            for hop in hops:
                far(hop, offset, a, place, place).wait_send()
            for hop in (0, *hops):
                near(hop, offset, a, place, place).wait_send()


def move(query_blocks, output_blocks, probes, shard_block, rep_count, multiply):
    tp_count, rows, cut = query_blocks.shape
    count = rep_count * tp_count
    half = rep_count // 2
    kinds = probes.shape[0]
    dma = pltpu.SemaphoreType.DMA
    anywhere = pl.BlockSpec(memory_space=pl.ANY)
    shapes = [
        jax.ShapeDtypeStruct((count, rows, cut), jnp.bfloat16),
        jax.ShapeDtypeStruct((count, cut, rows), jnp.bfloat16),
    ]
    scratch = [
        dma((2, tp_count)), dma((2, tp_count)),
        dma((half, 2, tp_count)), dma((half, 2, tp_count)),
        dma((half - 1, 2, tp_count)), dma((half - 1, 2, tp_count)),
        dma((2,)),
    ]
    operands, in_specs, out_specs = [query_blocks, output_blocks], [anywhere] * 2, [anywhere] * 2
    if multiply:
        operands = [shard_block] + operands + [probes]
        in_specs = [pl.BlockSpec(memory_space=pltpu.SMEM)] + [anywhere] * 3
        out_specs += [pl.BlockSpec(memory_space=pltpu.VMEM)] * 2
        shapes += [
            jax.ShapeDtypeStruct((1, kinds, cut), jnp.float32),
            jax.ShapeDtypeStruct((1, cut, kinds), jnp.float32),
        ]
        scratch += [
            pltpu.VMEM((count, kinds, rows), jnp.bfloat16),
            pltpu.VMEM((kinds, rep_count * rows), jnp.bfloat16),
            pltpu.VMEM((rep_count * rows, cut), jnp.bfloat16),
            pltpu.VMEM((cut, rep_count * rows), jnp.bfloat16),
            dma((2, rep_count)),
            dma((count,)),
        ]
    return pl.pallas_call(
        functools.partial(move_kernel, rep_count, tp_count, multiply),
        out_shape=shapes,
        in_specs=in_specs,
        out_specs=out_specs,
        scratch_shapes=scratch,
        compiler_params=pltpu.CompilerParams(collective_id=0, has_side_effects=True),
    )(*operands)


def order_kernel(group, inverse_ref, *refs):
    queries, outputs = refs[:group], refs[group : 2 * group]
    query_slice, output_slice = refs[2 * group :]
    rows = queries[0].shape[1]
    for j in range(group):
        query_slice[0, j * rows : (j + 1) * rows, :] = queries[j][0]
        output_slice[0, :, j * rows : (j + 1) * rows] = outputs[j][0]


def order(query_all, output_all, inverse):
    count, rows, cut = query_all.shape
    group = max(1, min(count, 1024 // rows))
    picks = range(group)
    return pl.pallas_call(
        functools.partial(order_kernel, group),
        out_shape=(
            jax.ShapeDtypeStruct((1, count * rows, cut), jnp.bfloat16),
            jax.ShapeDtypeStruct((1, cut, count * rows), jnp.bfloat16),
        ),
        grid_spec=pltpu.PrefetchScalarGridSpec(
            num_scalar_prefetch=1,
            grid=(count // group,),
            in_specs=[
                pl.BlockSpec((1, rows, cut), lambda b, inv, j=j: (inv[b * group + j], 0, 0))
                for j in picks
            ]
            + [
                pl.BlockSpec((1, cut, rows), lambda b, inv, j=j: (inv[b * group + j], 0, 0))
                for j in picks
            ],
            out_specs=[
                pl.BlockSpec((1, group * rows, cut), lambda b, inv: (0, b, 0)),
                pl.BlockSpec((1, cut, group * rows), lambda b, inv: (0, 0, b)),
            ],
        ),
    )(inverse, *([query_all] * group), *([output_all] * group))


def query_kernel(group, inverse_ref, *refs):
    blocks, (probes_ref, slice_ref, prints_ref) = refs[:group], refs[group:]
    rows = blocks[0].shape[1]
    for j, block in enumerate(blocks):
        slice_ref[0, j * rows : (j + 1) * rows, :] = block[0]
    part = jnp.dot(probes_ref[...], slice_ref[0], preferred_element_type=jnp.float32)

    @pl.when(pl.program_id(0) == 0)
    def _():
        prints_ref[0] = part

    @pl.when(pl.program_id(0) > 0)
    def _():
        prints_ref[0] += part


def output_kernel(group, inverse_ref, *refs):
    blocks, (probes_ref, slice_ref, prints_ref) = refs[:group], refs[group:]
    rows = blocks[0].shape[2]
    for j, block in enumerate(blocks):
        slice_ref[0, :, j * rows : (j + 1) * rows] = block[0]
    part = lax.dot_general(
        slice_ref[0], probes_ref[...], (((1,), (1,)), ((), ())),
        preferred_element_type=jnp.float32,
    )

    @pl.when(pl.program_id(0) == 0)
    def _():
        prints_ref[0] = part

    @pl.when(pl.program_id(0) > 0)
    def _():
        prints_ref[0] += part


def finish(body, everything, probes, inverse, slice_shape, prints_shape, along):
    count = everything.shape[0]
    block = everything.shape[1:]
    group = max(1, min(count, 1024 // block[along]))
    span = group * block[along]
    tile = list((1,) + block)
    tile[1 + along] = span
    in_specs = [
        pl.BlockSpec((1,) + block, lambda b, inv, j=j: (inv[b * group + j], 0, 0))
        for j in range(group)
    ]
    in_specs.append(pl.BlockSpec((probes.shape[0], span), lambda b, inv: (0, b)))
    place = (lambda b, inv: (0, b, 0)) if along == 0 else (lambda b, inv: (0, 0, b))
    return pl.pallas_call(
        functools.partial(body, group),
        out_shape=(
            jax.ShapeDtypeStruct(slice_shape, jnp.bfloat16),
            jax.ShapeDtypeStruct(prints_shape, jnp.float32),
        ),
        grid_spec=pltpu.PrefetchScalarGridSpec(
            num_scalar_prefetch=1,
            grid=(count // group,),
            in_specs=in_specs,
            out_specs=[
                pl.BlockSpec(tuple(tile), place),
                pl.BlockSpec(prints_shape, lambda b, inv: (0, 0, 0)),
            ],
        ),
    )(inverse, *([everything] * group), probes)


def stream_kernel(shard_ref, owner_ref, query_ref, output_ref, probes_ref,
                  query_all, output_all, query_prints, output_prints,
                  stage_even, stage_odd, query_out, output_out, probes, picked, query_tile, output_tile,
                  stage_sem, probes_sem, swap_send, swap_recv, far_send, far_recv,
                  near_send, near_recv):
    rep_count, tp_count = lax.axis_size("rep"), lax.axis_size("tp")
    rep, tp = lax.axis_index("rep"), lax.axis_index("tp")
    count, rows, cut = query_all.shape
    half = tp_count // 2
    parts = cut // stage_even.shape[2]
    size = stage_even.shape[2]
    partner = rep + 1 - 2 * lax.rem(rep, 2)
    facing = lax.rem(rep + 2, rep_count)
    behind = facing + 1 - 2 * lax.rem(facing, 2)
    mine = rep * tp_count + tp
    inner = lax.rem(lax.div(lax.div(tp, 2) + 1, 2), 2)
    everything = (query_all, output_all)
    stage = (stage_even, stage_odd)
    outgoing = (query_out, output_out)
    ticks = half * parts
    first = half + 1

    def pair(offset):
        return pair_index(tp, jnp.int32(offset), tp_count)

    def spot(a, part):
        piece = pl.ds(pl.multiple_of(part * size, size), size)
        return (slice(None), piece) if a == 0 else (piece, slice(None))

    def remote(source, target, send_sem, recv_sem, device):
        return pltpu.make_async_remote_copy(
            src_ref=source, dst_ref=target, send_sem=send_sem, recv_sem=recv_sem,
            device_id=device, device_id_type=MESH,
        )

    def swap(a, offset, part):
        return remote(
            outgoing[a].at[(offset - 1, *spot(a, part))],
            everything[a].at[(mine, *spot(a, part))],
            swap_send.at[a], swap_recv.at[a, offset, part], (rep, pair(offset)),
        )

    def held(group, a, offset, part):
        return everything[a].at[(group * tp_count + pair(offset), *spot(a, part))]

    def far(a, offset, part):
        place = held(rep, a, offset, part)
        return remote(place, place, far_send.at[a], far_recv.at[a, offset, part], (facing, tp))

    def near(kind, a, offset, part):
        place = held((rep, facing)[kind], a, offset, part)
        return remote(
            place, place, near_send.at[kind, a], near_recv.at[kind, a, offset, part],
            (partner, tp),
        )

    def load(a, part, h):
        copies = []
        depth = size // 2
        for k in range(tp_count):
            if a == 0:
                piece = pl.ds(pl.multiple_of(k * cut + part * size, size), size)
                source = query_ref.at[0, h * rows // 2 : (h + 1) * rows // 2, piece]
            else:
                piece = pl.ds(pl.multiple_of(k * cut + part * size + h * depth, depth), depth)
                source = output_ref.at[0, piece, :]
            copies.append(pltpu.make_async_copy(source, stage[h].at[k], stage_sem.at[h, k]))
        return copies

    def start_load(a, part, h):
        for copy in load(a, part, h):
            copy.start()

    def convert(a, part):
        if True:
            for h in range(2):
                for copy in load(a, part, h):
                    copy.wait()
                if a == 0:
                    piece = pl.ds(pl.multiple_of(part * size, size), size)
                    where = (slice(h * rows // 2, (h + 1) * rows // 2), piece)
                else:
                    depth = size // 2
                    piece = pl.ds(pl.multiple_of(part * size + h * depth, depth), depth)
                    where = (piece, slice(None))
                everything[a][(mine, *where)] = stage[h][owner_ref[tp]].astype(jnp.bfloat16)

                @pl.loop(1, tp_count)
                def _(offset):
                    outgoing[a][(offset - 1, *where)] = stage[h][
                        owner_ref[pair(offset)]
                    ].astype(jnp.bfloat16)

                if a == 0:
                    start_load(1, part, h)
                else:

                    @pl.when(part < parts - 1)
                    def _():
                        start_load(0, part + 1, h)

    def far_offset(e):
        return half + 2 * (1 - lax.rem(e, 2)) + lax.div(e, 2)

    def spread(a, offset, part):
        far(a, offset, part).start()
        near(0, a, offset, part).start()

    def send_near(a, part):
        @pl.loop(1, half)
        def _(offset):
            swap(a, offset, part).start()

    def send_far(a, n):
        swap(a, far_offset(lax.rem(n, half)), lax.div(n, half)).start()

    def near_item(k):
        shifted = k + half - 1 + lax.div(k, 3 * half + 1)
        j = lax.rem(shifted, half)
        part = lax.div(shifted, half) - lax.min(j, 1)
        return j * lax.min(k, 1), lax.max(part, 0)

    def item(p):
        late = lax.div(p, 2 * ticks - first)
        begun = lax.div(p + 2 * ticks - first, 2 * ticks)
        middle = lax.div(p + 2 * half - first, 2) - half
        is_far = begun * (late + (1 - late) * lax.rem(p, 2))
        n = is_far * (late * (p - ticks) + (1 - late) * middle)
        k = (1 - is_far) * (begun * (first + middle) + (1 - begun) * p)
        near_offset, near_part = near_item(k)
        offset = is_far * far_offset(lax.rem(n, half)) + (1 - is_far) * near_offset
        return offset, is_far * lax.div(n, half) + (1 - is_far) * near_part

    def relay(p):
        offset, part = item(p)
        for a in range(2):
            far(a, offset, part).wait_recv()
            near(1, a, offset, part).start()

    def collect(p):
        offset, part = item(p)
        groups = (rep, partner, facing, behind)
        for a in range(2):
            for kind in range(2):
                near(kind, a, offset, part).wait_recv()
        for g, group in enumerate(groups):
            source = group * tp_count + pair(offset)
            strip = slice(g * rows, (g + 1) * rows)
            picked[:, strip] = probes[shard_ref[source]]
            query_tile[strip, :] = query_all[(source, *spot(0, part))]
            output_tile[:, strip] = output_all[(source, *spot(1, part))]
        query_prints[(0, *spot(0, part))] += jnp.dot(
            picked[...], query_tile[...], preferred_element_type=jnp.float32
        )
        output_prints[(0, *spot(1, part))] += lax.dot_general(
            output_tile[...], picked[...], (((1,), (1,)), ((), ())),
            preferred_element_type=jnp.float32,
        )

    def load_probes(block):
        columns = pl.ds(pl.multiple_of(block * rows, rows), rows)
        return pltpu.make_async_copy(
            probes_ref.at[:, columns], probes.at[block], probes_sem.at[block]
        )

    for h in range(2):
        start_load(0, 0, h)
    barrier = pltpu.get_barrier_semaphore()
    peers = [(rep, pair(offset)) for offset in range(1, tp_count)]
    peers += [(partner, tp), (facing, tp)]
    for peer in peers:
        pl.semaphore_signal(barrier, inc=1, device_id=peer, device_id_type=MESH)
    for a in range(2):
        convert(a, jnp.int32(0))
        if a == 0:
            pl.semaphore_wait(barrier, len(peers))
        spread(a, jnp.int32(0), 0)

        @pl.when(inner == 1)
        def _():
            for n in range(LEAD):
                send_far(a, jnp.int32(n))

        send_near(a, 0)

        @pl.when(inner == 0)
        def _():
            for n in range(LEAD):
                send_far(a, jnp.int32(n))

    for a in range(2):
        convert(a, jnp.int32(1))
        spread(a, jnp.int32(0), 1)
        send_near(a, 1)

    @pl.loop(0, count)
    def _(block):
        load_probes(block).start()

    query_prints[...] = jnp.zeros_like(query_prints)
    output_prints[...] = jnp.zeros_like(output_prints)
    for a in range(2):
        convert(a, jnp.int32(2))

    @pl.loop(1, half)
    def _(offset):
        for a in range(2):
            swap(a, offset, 0).wait_recv()
            spread(a, offset, 0)

    @pl.loop(0, count)
    def _(block):
        load_probes(block).wait()

    @pl.loop(0, ticks + 2 + LAG)
    def _(m):
        @pl.loop(0, 2)
        def _(i):
            p = 2 * (m - LAG) - 3 + i

            @pl.when((p >= 0) & (p < 2 * ticks))
            def _():
                collect(p)

        @pl.when(m < ticks)
        def _():
            offset, part = far_offset(lax.rem(m, half)), lax.div(m, half)
            for a in range(2):
                swap(a, offset, part).wait_recv()
                spread(a, offset, part)

            @pl.when(m < ticks - LEAD)
            def _():
                for a in range(2):
                    send_far(a, m + LEAD)

        @pl.when(m < ticks - first)
        def _():
            offset, part = near_item(first + m)
            for a in range(2):

                @pl.when(offset > 0)
                def _():
                    swap(a, lax.max(offset, 1), part).wait_recv()

                spread(a, offset, part)

        @pl.when(m == 0)
        def _():
            for a in range(2):
                convert(a, jnp.int32(parts - 1))

        @pl.when((m == 1) | (m == half))
        def _():
            for a in range(2):
                send_near(a, 2 + lax.div(m, half))

        @pl.loop(0, 2)
        def _(i):
            p = 2 * (m - LAG) - 1 + i

            @pl.when((p >= 0) & (p < 2 * ticks))
            def _():
                relay(p)

    for a in range(2):
        whole = outgoing[a]
        remote(whole, whole, swap_send.at[a], swap_recv.at[a, 0, 0], (partner, tp)).wait_send()
        whole = everything[a].at[pl.ds(0, tp_count)]
        for sem in (far_send.at[a], near_send.at[0, a], near_send.at[1, a]):
            remote(whole, whole, sem, swap_recv.at[a, 0, 0], (partner, tp)).wait_send()


def stream(trainer_query, trainer_output, probes, shard_block, slice_owner, rep_count):
    tp_count = slice_owner.shape[0]
    _, rows, width = trainer_query.shape
    cut = width // tp_count
    count = rep_count * tp_count
    kinds = probes.shape[0]
    parts = 4
    size = cut // parts
    dma = pltpu.SemaphoreType.DMA
    anywhere = pl.BlockSpec(memory_space=pl.ANY)
    small = pl.BlockSpec(memory_space=pltpu.SMEM)
    depth = rep_count * rows
    return pl.pallas_call(
        stream_kernel,
        out_shape=[
            pltpu.VMEM((count, rows, cut), jnp.bfloat16),
            pltpu.VMEM((count, cut, rows), jnp.bfloat16),
            pltpu.VMEM((1, kinds, cut), jnp.float32),
            pltpu.VMEM((1, cut, kinds), jnp.float32),
        ],
        in_specs=[small, small, anywhere, anywhere, anywhere],
        out_specs=[pl.BlockSpec(memory_space=pltpu.VMEM)] * 4,
        scratch_shapes=[
            pltpu.VMEM((tp_count, size // 2, size), jnp.float32),
            pltpu.VMEM((tp_count, size // 2, size), jnp.float32),
            pltpu.VMEM((tp_count - 1, rows, cut), jnp.bfloat16),
            pltpu.VMEM((tp_count - 1, cut, rows), jnp.bfloat16),
            pltpu.VMEM((count, kinds, rows), jnp.bfloat16),
            pltpu.VMEM((kinds, depth), jnp.bfloat16),
            pltpu.VMEM((depth, size), jnp.bfloat16),
            pltpu.VMEM((size, depth), jnp.bfloat16),
            dma((2, tp_count)), dma((count,)),
            dma((2,)), dma((2, tp_count, parts)),
            dma((2,)), dma((2, tp_count, parts)),
            dma((2, 2)), dma((2, 2, tp_count, parts)),
        ],
        compiler_params=pltpu.CompilerParams(
            collective_id=0, has_side_effects=True, vmem_limit_bytes=VMEM_LIMIT
        ),
    )(shard_block, slice_owner, trainer_query, trainer_output, probes)


def place_kernel(shard_ref, query_all, output_all, query_prints, output_prints,
                 query_slice, output_slice, query_result, output_result, sems):
    count, rows, _ = query_all.shape

    @pl.loop(0, count)
    def _(source):
        block = pl.ds(pl.multiple_of(shard_ref[source] * rows, rows), rows)
        pltpu.make_async_copy(
            query_all.at[source], query_slice.at[0, block, :], sems.at[0]
        ).start()
        pltpu.make_async_copy(
            output_all.at[source], output_slice.at[0, :, block], sems.at[1]
        ).start()

    prints = (
        pltpu.make_async_copy(query_prints, query_result, sems.at[2]),
        pltpu.make_async_copy(output_prints, output_result, sems.at[3]),
    )
    for copy in prints:
        copy.start()
    for k, everything in enumerate((query_all, output_all)):
        pltpu.make_async_copy(everything, everything, sems.at[k]).wait()
    for copy in prints:
        copy.wait()


def place(moved, shard_block):
    query_all, output_all, query_prints, output_prints = moved
    count, rows, cut = query_all.shape
    inside = pl.BlockSpec(memory_space=pltpu.VMEM)
    return pl.pallas_call(
        place_kernel,
        out_shape=(
            jax.ShapeDtypeStruct((1, count * rows, cut), jnp.bfloat16),
            jax.ShapeDtypeStruct((1, cut, count * rows), jnp.bfloat16),
            jax.ShapeDtypeStruct(query_prints.shape, jnp.float32),
            jax.ShapeDtypeStruct(output_prints.shape, jnp.float32),
        ),
        in_specs=[pl.BlockSpec(memory_space=pltpu.SMEM)] + [inside] * 4,
        out_specs=[pl.BlockSpec(memory_space=pl.ANY)] * 4,
        scratch_shapes=[pltpu.SemaphoreType.DMA((4,))],
        compiler_params=pltpu.CompilerParams(vmem_limit_bytes=VMEM_LIMIT),
    )(shard_block, *(pltpu.with_memory_space_constraint(x, pltpu.VMEM) for x in moved))


def per_device(trainer_query, trainer_output, probes, shard_block, slice_owner):
    tp_count = lax.axis_size("tp")
    rep_count = lax.axis_size("rep")
    count = tp_count * rep_count
    rows, width = trainer_query.shape[1:]
    cut = width // tp_count
    model = rows * count
    if rep_count == 4 and tp_count == 8 and rows % 128 == 0 and cut == 4 * rows:
        moved = stream(
            trainer_query, trainer_output, probes, shard_block, slice_owner, rep_count
        )
        return place(moved, shard_block)
    positions = jnp.arange(count, dtype=jnp.int32)
    held = shard_block[None, :] == positions[:, None]
    inverse = jnp.sum(jnp.where(held, positions[None, :], 0), axis=1, dtype=jnp.int32)
    query_blocks, output_blocks = pack(trainer_query, trainer_output, slice_owner)
    multiply = rows % 128 == 0
    moved = move(query_blocks, output_blocks, probes, shard_block, rep_count, multiply)
    if multiply:
        query_all, output_all, query_prints, output_prints = moved
        query_slice, output_slice = order(query_all, output_all, inverse)
        return query_slice, output_slice, query_prints, output_prints
    query_all, output_all = moved
    query_slice, query_prints = finish(
        query_kernel, query_all, probes, inverse,
        (1, model, cut), (1, probes.shape[0], cut), 0,
    )
    output_slice, output_prints = finish(
        output_kernel, output_all, probes, inverse,
        (1, cut, model), (1, cut, probes.shape[0]), 1,
    )
    return query_slice, output_slice, query_prints, output_prints


def solution(mesh):
    placed = (P(("rep", "tp"), None, None), P(("rep", "tp"), None, None), P(), P(), P())
    return jax.shard_map(
        per_device,
        mesh=mesh,
        in_specs=placed,
        out_specs=(
            P("tp", None, None),
            P("tp", None, None),
            P("tp", None, None),
            P("tp", None, None),
        ),
        check_vma=False,
    )
```

```python
import functools

import jax
import jax.numpy as jnp
from jax import lax
from jax.experimental import pallas as pl
from jax.experimental.pallas import tpu as pltpu
from jax.sharding import PartitionSpec as P

MESH = pl.DeviceIdType.MESH
VMEM_LIMIT = 51 * 256 * 1024
LEAD = 6
LAG = 1


def pack_kernel(owner_ref, query_ref, output_ref, query_blocks, output_blocks):
    query_blocks[...] = query_ref[...].astype(jnp.bfloat16)
    output_blocks[...] = output_ref[...].astype(jnp.bfloat16)


def pack(trainer_query, trainer_output, slice_owner):
    tp_count = slice_owner.shape[0]
    _, rows, width = trainer_query.shape
    cut = width // tp_count
    return pl.pallas_call(
        pack_kernel,
        out_shape=(
            jax.ShapeDtypeStruct((tp_count, rows, cut), jnp.bfloat16),
            jax.ShapeDtypeStruct((tp_count, cut, rows), jnp.bfloat16),
        ),
        grid_spec=pltpu.PrefetchScalarGridSpec(
            num_scalar_prefetch=1,
            grid=(tp_count,),
            in_specs=[
                pl.BlockSpec((1, rows, cut), lambda k, owner: (0, 0, owner[k])),
                pl.BlockSpec((1, cut, rows), lambda k, owner: (0, owner[k], 0)),
            ],
            out_specs=[
                pl.BlockSpec((1, rows, cut), lambda k, owner: (k, 0, 0)),
                pl.BlockSpec((1, cut, rows), lambda k, owner: (k, 0, 0)),
            ],
        ),
    )(slice_owner, trainer_query, trainer_output)


def pair_index(index, offset, count):
    paired, bit = 0, 1
    while bit < count:
        low = lax.rem(lax.div(index, bit) + lax.div(offset, bit), 2)
        paired = paired + bit * low
        bit *= 2
    return paired


def move_kernel(rep_count, tp_count, multiply, *refs):
    if multiply:
        (owner_ref, query_blocks, output_blocks, probes_ref,
         query_all, output_all, query_prints, output_prints,
         swap_send, swap_recv, near_send, near_recv, far_send, far_recv, own_sem,
         probes, picked, query_tile, output_tile, load_sem, probes_sem) = refs
    else:
        (query_blocks, output_blocks, query_all, output_all,
         swap_send, swap_recv, near_send, near_recv, far_send, far_recv, own_sem) = refs
    rep, tp = lax.axis_index("rep"), lax.axis_index("tp")
    partner = rep + 1 - 2 * lax.rem(rep, 2)
    hops = range(1, rep_count // 2)
    ahead = {hop: lax.rem(rep + 2 * hop, rep_count) for hop in hops}
    behind = {hop: lax.rem(rep + rep_count - 2 * hop, rep_count) for hop in hops}
    across = {hop: lax.rem(partner + rep_count - 2 * hop, rep_count) for hop in hops}
    arrays = ((query_blocks, query_all), (output_blocks, output_all))
    mine = rep * tp_count + tp
    count = rep_count * tp_count
    rows = query_blocks.shape[1]

    def load_probes(block):
        columns = pl.ds(pl.multiple_of(block * rows, rows), rows)
        return pltpu.make_async_copy(
            probes_ref.at[:, columns], probes.at[block], probes_sem.at[block]
        )

    def pair(offset):
        return pair_index(tp, jnp.int32(offset), tp_count)

    barrier = pltpu.get_barrier_semaphore()
    peers = [(rep, pair(offset)) for offset in range(1, tp_count)]
    peers += [(partner, tp)] + [(ahead[hop], tp) for hop in hops]
    for peer in peers:
        pl.semaphore_signal(barrier, inc=1, device_id=peer, device_id_type=MESH)
    pl.semaphore_wait(barrier, len(peers))

    def remote(source, target, send_sem, recv_sem, device):
        return pltpu.make_async_remote_copy(
            src_ref=source, dst_ref=target, send_sem=send_sem, recv_sem=recv_sem,
            device_id=device, device_id_type=MESH,
        )

    def swap(offset, a):
        blocks, everything = arrays[a]
        return remote(
            blocks.at[pair(offset)], everything.at[mine],
            swap_send.at[a, offset], swap_recv.at[a, offset], (rep, pair(offset)),
        )

    def far(hop, offset, a, block, place):
        return remote(
            block, place, far_send.at[hop - 1, a, offset], far_recv.at[hop - 1, a, offset],
            (ahead[hop], tp),
        )

    def near(hop, offset, a, block, place):
        return remote(
            block, place, near_send.at[hop, a, offset], near_recv.at[hop, a, offset],
            (partner, tp),
        )

    def place_of(group, offset, a):
        return arrays[a][1].at[group * tp_count + pair(offset)]

    def own(a):
        blocks, everything = arrays[a]
        return pltpu.make_async_copy(blocks.at[tp], everything.at[mine], own_sem.at[a])

    def spread(offset, a, block):
        place = place_of(rep, offset, a)
        for hop in hops:
            far(hop, offset, a, block, place).start()
        near(0, offset, a, block, place).start()

    def relay(offset, a):
        for hop in hops:
            place = place_of(behind[hop], offset, a)
            far(hop, offset, a, place, place).wait_recv()
            near(hop, offset, a, place, place).start()

    def collect(offset, a):
        for hop in (0, *hops):
            place = place_of(rep, offset, a)
            near(hop, offset, a, place, place).wait_recv()

        @pl.when(offset == 0)
        def _():
            own(a).wait()
            if multiply and a == 0:

                @pl.loop(0, count)
                def _(block):
                    load_probes(block).wait()


        if not multiply:
            return
        groups = [rep, partner]
        for hop in hops:
            groups += [behind[hop], across[hop]]
        tile, prints = ((query_tile, query_prints), (output_tile, output_prints))[a]
        loads = []
        for j, group in enumerate(groups):
            spot = (pl.ds(j * rows, rows), slice(None))
            load = pltpu.make_async_copy(
                place_of(group, offset, a), tile.at[spot if a == 0 else spot[::-1]],
                load_sem.at[a, j],
            )
            load.start()
            loads.append(load)
        for j, group in enumerate(groups):
            owner = owner_ref[group * tp_count + pair(offset)]
            picked[:, j * rows : (j + 1) * rows] = probes[owner]
        for load in loads:
            load.wait()
        if a == 0:
            prints[0] += jnp.dot(picked[...], tile[...], preferred_element_type=jnp.float32)
        else:
            prints[0] += lax.dot_general(
                tile[...], picked[...], (((1,), (1,)), ((), ())),
                preferred_element_type=jnp.float32,
            )

    for offset in range(1, tp_count):
        for a in range(2):
            swap(offset, a).start()
    for a in range(2):
        spread(jnp.int32(0), a, arrays[a][0].at[tp])
    for a in range(2):
        own(a).start()
    if multiply:

        @pl.loop(0, count)
        def _(block):
            load_probes(block).start()

        query_prints[...] = jnp.zeros_like(query_prints)
        output_prints[...] = jnp.zeros_like(output_prints)

    @pl.loop(1, tp_count + 2)
    def _(step):
        for a in range(2):

            @pl.when(step < tp_count)
            def _():
                swap(step, a).wait_recv()
                spread(step, a, place_of(rep, step, a))

            @pl.when(step <= tp_count)
            def _():
                relay(step - 1, a)

            if a == 0:

                @pl.when(step >= 2)
                def _():
                    collect(step - 2, 1)

            else:

                @pl.when(step <= tp_count)
                def _():
                    collect(step - 1, 0)

    @pl.loop(0, tp_count)
    def _(offset):
        for a in range(2):

            @pl.when(offset > 0)
            def _():
                swap(offset, a).wait_send()

            place = place_of(rep, offset, a)
            for hop in hops:
                far(hop, offset, a, place, place).wait_send()
            for hop in (0, *hops):
                near(hop, offset, a, place, place).wait_send()


def move(query_blocks, output_blocks, probes, shard_block, rep_count, multiply):
    tp_count, rows, cut = query_blocks.shape
    count = rep_count * tp_count
    half = rep_count // 2
    kinds = probes.shape[0]
    dma = pltpu.SemaphoreType.DMA
    anywhere = pl.BlockSpec(memory_space=pl.ANY)
    shapes = [
        jax.ShapeDtypeStruct((count, rows, cut), jnp.bfloat16),
        jax.ShapeDtypeStruct((count, cut, rows), jnp.bfloat16),
    ]
    scratch = [
        dma((2, tp_count)), dma((2, tp_count)),
        dma((half, 2, tp_count)), dma((half, 2, tp_count)),
        dma((half - 1, 2, tp_count)), dma((half - 1, 2, tp_count)),
        dma((2,)),
    ]
    operands, in_specs, out_specs = [query_blocks, output_blocks], [anywhere] * 2, [anywhere] * 2
    if multiply:
        operands = [shard_block] + operands + [probes]
        in_specs = [pl.BlockSpec(memory_space=pltpu.SMEM)] + [anywhere] * 3
        out_specs += [pl.BlockSpec(memory_space=pltpu.VMEM)] * 2
        shapes += [
            jax.ShapeDtypeStruct((1, kinds, cut), jnp.float32),
            jax.ShapeDtypeStruct((1, cut, kinds), jnp.float32),
        ]
        scratch += [
            pltpu.VMEM((count, kinds, rows), jnp.bfloat16),
            pltpu.VMEM((kinds, rep_count * rows), jnp.bfloat16),
            pltpu.VMEM((rep_count * rows, cut), jnp.bfloat16),
            pltpu.VMEM((cut, rep_count * rows), jnp.bfloat16),
            dma((2, rep_count)),
            dma((count,)),
        ]
    return pl.pallas_call(
        functools.partial(move_kernel, rep_count, tp_count, multiply),
        out_shape=shapes,
        in_specs=in_specs,
        out_specs=out_specs,
        scratch_shapes=scratch,
        compiler_params=pltpu.CompilerParams(collective_id=0, has_side_effects=True),
    )(*operands)


def order_kernel(group, inverse_ref, *refs):
    queries, outputs = refs[:group], refs[group : 2 * group]
    query_slice, output_slice = refs[2 * group :]
    rows = queries[0].shape[1]
    for j in range(group):
        query_slice[0, j * rows : (j + 1) * rows, :] = queries[j][0]
        output_slice[0, :, j * rows : (j + 1) * rows] = outputs[j][0]


def order(query_all, output_all, inverse):
    count, rows, cut = query_all.shape
    group = max(1, min(count, 1024 // rows))
    picks = range(group)
    return pl.pallas_call(
        functools.partial(order_kernel, group),
        out_shape=(
            jax.ShapeDtypeStruct((1, count * rows, cut), jnp.bfloat16),
            jax.ShapeDtypeStruct((1, cut, count * rows), jnp.bfloat16),
        ),
        grid_spec=pltpu.PrefetchScalarGridSpec(
            num_scalar_prefetch=1,
            grid=(count // group,),
            in_specs=[
                pl.BlockSpec((1, rows, cut), lambda b, inv, j=j: (inv[b * group + j], 0, 0))
                for j in picks
            ]
            + [
                pl.BlockSpec((1, cut, rows), lambda b, inv, j=j: (inv[b * group + j], 0, 0))
                for j in picks
            ],
            out_specs=[
                pl.BlockSpec((1, group * rows, cut), lambda b, inv: (0, b, 0)),
                pl.BlockSpec((1, cut, group * rows), lambda b, inv: (0, 0, b)),
            ],
        ),
    )(inverse, *([query_all] * group), *([output_all] * group))


def query_kernel(group, inverse_ref, *refs):
    blocks, (probes_ref, slice_ref, prints_ref) = refs[:group], refs[group:]
    rows = blocks[0].shape[1]
    for j, block in enumerate(blocks):
        slice_ref[0, j * rows : (j + 1) * rows, :] = block[0]
    part = jnp.dot(probes_ref[...], slice_ref[0], preferred_element_type=jnp.float32)

    @pl.when(pl.program_id(0) == 0)
    def _():
        prints_ref[0] = part

    @pl.when(pl.program_id(0) > 0)
    def _():
        prints_ref[0] += part


def output_kernel(group, inverse_ref, *refs):
    blocks, (probes_ref, slice_ref, prints_ref) = refs[:group], refs[group:]
    rows = blocks[0].shape[2]
    for j, block in enumerate(blocks):
        slice_ref[0, :, j * rows : (j + 1) * rows] = block[0]
    part = lax.dot_general(
        slice_ref[0], probes_ref[...], (((1,), (1,)), ((), ())),
        preferred_element_type=jnp.float32,
    )

    @pl.when(pl.program_id(0) == 0)
    def _():
        prints_ref[0] = part

    @pl.when(pl.program_id(0) > 0)
    def _():
        prints_ref[0] += part


def finish(body, everything, probes, inverse, slice_shape, prints_shape, along):
    count = everything.shape[0]
    block = everything.shape[1:]
    group = max(1, min(count, 1024 // block[along]))
    span = group * block[along]
    tile = list((1,) + block)
    tile[1 + along] = span
    in_specs = [
        pl.BlockSpec((1,) + block, lambda b, inv, j=j: (inv[b * group + j], 0, 0))
        for j in range(group)
    ]
    in_specs.append(pl.BlockSpec((probes.shape[0], span), lambda b, inv: (0, b)))
    place = (lambda b, inv: (0, b, 0)) if along == 0 else (lambda b, inv: (0, 0, b))
    return pl.pallas_call(
        functools.partial(body, group),
        out_shape=(
            jax.ShapeDtypeStruct(slice_shape, jnp.bfloat16),
            jax.ShapeDtypeStruct(prints_shape, jnp.float32),
        ),
        grid_spec=pltpu.PrefetchScalarGridSpec(
            num_scalar_prefetch=1,
            grid=(count // group,),
            in_specs=in_specs,
            out_specs=[
                pl.BlockSpec(tuple(tile), place),
                pl.BlockSpec(prints_shape, lambda b, inv: (0, 0, 0)),
            ],
        ),
    )(inverse, *([everything] * group), probes)


def stream_kernel(shard_ref, owner_ref, query_ref, output_ref, probes_ref,
                  query_all, output_all, query_prints, output_prints, probes,
                  stage_even, stage_odd, query_out, output_out, picked, query_tile, output_tile,
                  stage_sem, probes_sem, swap_send, swap_recv, far_send, far_recv,
                  near_send, near_recv):
    rep_count, tp_count = lax.axis_size("rep"), lax.axis_size("tp")
    rep, tp = lax.axis_index("rep"), lax.axis_index("tp")
    count, rows, cut = query_all.shape
    half = tp_count // 2
    size = stage_even.shape[2]
    strips = cut // size
    step = size // 2
    parts = cut // step
    partner = rep + 1 - 2 * lax.rem(rep, 2)
    facing = lax.rem(rep + 2, rep_count)
    behind = facing + 1 - 2 * lax.rem(facing, 2)
    mine = rep * tp_count + tp
    inner = lax.rem(lax.div(lax.div(tp, 2) + 1, 2), 2)
    everything = (query_all, output_all)
    stage = (stage_even, stage_odd)
    outgoing = (query_out, output_out)
    ticks = half * parts
    first = half + 2 * (half - 1)

    def pair(offset):
        return pair_index(tp, jnp.int32(offset), tp_count)

    def spot(a, part, size=step):
        piece = pl.ds(pl.multiple_of(part * size, size), size)
        return (slice(None), piece) if a == 0 else (piece, slice(None))

    def remote(source, target, send_sem, recv_sem, device):
        return pltpu.make_async_remote_copy(
            src_ref=source, dst_ref=target, send_sem=send_sem, recv_sem=recv_sem,
            device_id=device, device_id_type=MESH,
        )

    def swap(a, offset, part):
        return remote(
            outgoing[a].at[(offset - 1, *spot(a, part))],
            everything[a].at[(mine, *spot(a, part))],
            swap_send.at[a], swap_recv.at[a, offset, part], (rep, pair(offset)),
        )

    def held(group, a, offset, part):
        return everything[a].at[(group * tp_count + pair(offset), *spot(a, part))]

    def far(a, offset, part):
        place = held(rep, a, offset, part)
        return remote(place, place, far_send.at[a], far_recv.at[a, offset, part], (facing, tp))

    def near(kind, a, offset, part):
        place = held((rep, facing)[kind], a, offset, part)
        return remote(
            place, place, near_send.at[kind, a], near_recv.at[kind, a, offset, part],
            (partner, tp),
        )

    def load(a, part, h):
        copies = []
        depth = size // 2
        for k in range(tp_count):
            if a == 0:
                piece = pl.ds(pl.multiple_of(k * cut + part * size, size), size)
                source = query_ref.at[0, h * rows // 2 : (h + 1) * rows // 2, piece]
            else:
                piece = pl.ds(pl.multiple_of(k * cut + part * size + h * depth, depth), depth)
                source = output_ref.at[0, piece, :]
            copies.append(pltpu.make_async_copy(source, stage[h].at[k], stage_sem.at[h, k]))
        return copies

    def start_load(a, part, h):
        for copy in load(a, part, h):
            copy.start()

    def convert(a, part):
        if True:
            for h in range(2):
                for copy in load(a, part, h):
                    copy.wait()
                if a == 0:
                    piece = pl.ds(pl.multiple_of(part * size, size), size)
                    where = (slice(h * rows // 2, (h + 1) * rows // 2), piece)
                else:
                    depth = size // 2
                    piece = pl.ds(pl.multiple_of(part * size + h * depth, depth), depth)
                    where = (piece, slice(None))
                everything[a][(mine, *where)] = stage[h][owner_ref[tp]].astype(jnp.bfloat16)

                @pl.loop(1, tp_count)
                def _(offset):
                    outgoing[a][(offset - 1, *where)] = stage[h][
                        owner_ref[pair(offset)]
                    ].astype(jnp.bfloat16)

                if a == 0:
                    start_load(1, part, h)
                else:

                    @pl.when(part < strips - 1)
                    def _():
                        start_load(0, part + 1, h)

    def far_offset(e):
        return half + 2 * (1 - lax.rem(e, 2)) + lax.div(e, 2)

    def spread(a, offset, part):
        far(a, offset, part).start()
        near(0, a, offset, part).start()

    def send_near(a, part):
        @pl.loop(1, half)
        def _(offset):
            swap(a, offset, part).start()

    def send_far(a, n):
        swap(a, far_offset(lax.rem(n, half)), lax.div(n, half)).start()

    def near_item(k):
        begun = lax.min(lax.div(k, half), 1)
        middle = lax.min(lax.div(k, first), 1)
        last = lax.min(lax.div(k, first + 4 * half), 1)
        j = lax.rem(k + 2, half)
        offset = (begun - middle) * (lax.rem(k + 2, half - 1) + 1)
        offset += (middle - last) * j
        offset += last * (lax.rem(k + 1, half - 1) + 1)
        part = (1 - begun) * k + (begun - middle) * (lax.div(k + 2, half - 1) - 2)
        part += (middle - last) * (lax.div(k + 2, half) + 1 - 2 * lax.min(j, 1))
        part += last * (lax.div(k + 1, half - 1) - 3)
        return offset, part

    def item(p):
        late = lax.div(p, 2 * ticks - first)
        begun = lax.div(p + 2 * ticks - first, 2 * ticks)
        middle = lax.div(p + first, 2) - first
        is_far = begun * (late + (1 - late) * (1 - lax.rem(p, 2)))
        n = is_far * (late * (p - ticks) + (1 - late) * middle)
        k = (1 - is_far) * (begun * (first + middle) + (1 - begun) * p)
        near_offset, near_part = near_item(k)
        offset = is_far * far_offset(lax.rem(n, half)) + (1 - is_far) * near_offset
        return offset, is_far * lax.div(n, half) + (1 - is_far) * near_part

    def relay(p):
        offset, part = item(p)
        for a in range(2):
            far(a, offset, part).wait_recv()
            near(1, a, offset, part).start()

    def collect(p):
        offset, part = item(p)
        groups = (rep, partner, facing, behind)
        for a in range(2):
            for kind in range(2):
                near(kind, a, offset, part).wait_recv()

        @pl.when((lax.rem(part, 2) == 1) & (p < 2 * ticks - half))
        def _():
            strip = lax.div(part, 2)
            for g, group in enumerate(groups):
                source = group * tp_count + pair(offset)
                along = slice(g * rows, (g + 1) * rows)
                picked[:, along] = probes[shard_ref[source]]
                query_tile[along, :] = query_all[(source, *spot(0, strip, size))]
                output_tile[:, along] = output_all[(source, *spot(1, strip, size))]
            query_prints[(0, *spot(0, strip, size))] += jnp.dot(
                picked[...], query_tile[...], preferred_element_type=jnp.float32
            )
            output_prints[(0, *spot(1, strip, size))] += lax.dot_general(
                output_tile[...], picked[...], (((1,), (1,)), ((), ())),
                preferred_element_type=jnp.float32,
            )

    def load_probes(block):
        columns = pl.ds(pl.multiple_of(block * rows, rows), rows)
        return pltpu.make_async_copy(
            probes_ref.at[:, columns], probes.at[block], probes_sem.at[block]
        )

    for h in range(2):
        start_load(0, 0, h)
    barrier = pltpu.get_barrier_semaphore()
    peers = [(rep, pair(offset)) for offset in range(1, tp_count)]
    peers += [(partner, tp), (facing, tp)]
    for peer in peers:
        pl.semaphore_signal(barrier, inc=1, device_id=peer, device_id_type=MESH)
    for a in range(2):
        convert(a, jnp.int32(0))
        if a == 0:
            pl.semaphore_wait(barrier, len(peers))
        for part in range(2):
            spread(a, jnp.int32(0), part)

        @pl.when(inner == 1)
        def _():
            for n in range(LEAD):
                send_far(a, jnp.int32(n))

        for part in range(2):
            send_near(a, part)

        @pl.when(inner == 0)
        def _():
            for n in range(LEAD):
                send_far(a, jnp.int32(n))

    for a in range(2):
        convert(a, jnp.int32(1))
        for part in range(2, 4):
            spread(a, jnp.int32(0), part)
        send_near(a, 2)

    @pl.loop(0, count)
    def _(block):
        load_probes(block).start()

    query_prints[...] = jnp.zeros_like(query_prints)
    output_prints[...] = jnp.zeros_like(output_prints)
    for a in range(2):
        convert(a, jnp.int32(2))

    @pl.loop(half, first)
    def _(k):
        offset, part = near_item(k)
        for a in range(2):
            swap(a, offset, part).wait_recv()
            spread(a, offset, part)

    @pl.loop(0, count)
    def _(block):
        load_probes(block).wait()

    @pl.loop(0, ticks + 2 + LAG)
    def _(m):
        @pl.loop(0, 2)
        def _(i):
            p = 2 * (m - LAG) - 3 + i

            @pl.when((p >= 0) & (p < 2 * ticks))
            def _():
                collect(p)

        @pl.when(m < ticks)
        def _():
            offset, part = far_offset(lax.rem(m, half)), lax.div(m, half)
            for a in range(2):
                swap(a, offset, part).wait_recv()
                spread(a, offset, part)

            @pl.when(m < ticks - LEAD)
            def _():
                for a in range(2):
                    send_far(a, m + LEAD)

        @pl.when(m < ticks - first)
        def _():
            offset, part = near_item(first + m)
            for a in range(2):

                @pl.when(offset > 0)
                def _():
                    swap(a, lax.max(offset, 1), part).wait_recv()

                spread(a, offset, part)

        @pl.when(m == 1)
        def _():
            for a in range(2):
                convert(a, jnp.int32(strips - 1))

        @pl.when((lax.rem(m, 3) == 0) & (m < 3 * (parts - 3)))
        def _():
            for a in range(2):
                send_near(a, 3 + lax.div(m, 3))

        @pl.loop(0, 2)
        def _(i):
            p = 2 * (m - LAG) - 1 + i

            @pl.when((p >= 0) & (p < 2 * ticks))
            def _():
                relay(p)

    for a in range(2):
        whole = outgoing[a]
        remote(whole, whole, swap_send.at[a], swap_recv.at[a, 0, 0], (partner, tp)).wait_send()
        whole = everything[a].at[pl.ds(0, tp_count)]
        for sem in (far_send.at[a], near_send.at[0, a], near_send.at[1, a]):
            remote(whole, whole, sem, swap_recv.at[a, 0, 0], (partner, tp)).wait_send()


def stream(trainer_query, trainer_output, probes, shard_block, slice_owner, rep_count):
    tp_count = slice_owner.shape[0]
    _, rows, width = trainer_query.shape
    cut = width // tp_count
    count = rep_count * tp_count
    kinds = probes.shape[0]
    size = cut // 4
    parts = 8
    dma = pltpu.SemaphoreType.DMA
    anywhere = pl.BlockSpec(memory_space=pl.ANY)
    small = pl.BlockSpec(memory_space=pltpu.SMEM)
    depth = rep_count * rows
    return pl.pallas_call(
        stream_kernel,
        out_shape=[
            pltpu.VMEM((count, rows, cut), jnp.bfloat16),
            pltpu.VMEM((count, cut, rows), jnp.bfloat16),
            pltpu.VMEM((1, kinds, cut), jnp.float32),
            pltpu.VMEM((1, cut, kinds), jnp.float32),
            pltpu.VMEM((count, kinds, rows), jnp.bfloat16),
        ],
        in_specs=[small, small, anywhere, anywhere, anywhere],
        out_specs=[pl.BlockSpec(memory_space=pltpu.VMEM)] * 5,
        scratch_shapes=[
            pltpu.VMEM((tp_count, size // 2, size), jnp.float32),
            pltpu.VMEM((tp_count, size // 2, size), jnp.float32),
            pltpu.VMEM((tp_count - 1, rows, cut), jnp.bfloat16),
            pltpu.VMEM((tp_count - 1, cut, rows), jnp.bfloat16),
            pltpu.VMEM((kinds, depth), jnp.bfloat16),
            pltpu.VMEM((depth, size), jnp.bfloat16),
            pltpu.VMEM((size, depth), jnp.bfloat16),
            dma((2, tp_count)), dma((count,)),
            dma((2,)), dma((2, tp_count, parts)),
            dma((2,)), dma((2, tp_count, parts)),
            dma((2, 2)), dma((2, 2, tp_count, parts)),
        ],
        compiler_params=pltpu.CompilerParams(
            collective_id=0, has_side_effects=True, vmem_limit_bytes=VMEM_LIMIT
        ),
    )(shard_block, slice_owner, trainer_query, trainer_output, probes)


def place_kernel(shard_ref, query_all, output_all, query_prints, output_prints, probes,
                 query_slice, output_slice, query_result, output_result,
                 query_last, output_last, picked, query_tile, output_tile, sems):
    rep_count, tp_count = lax.axis_size("rep"), lax.axis_size("tp")
    tp = lax.axis_index("tp")
    count, rows, cut = query_all.shape
    size = query_tile.shape[1]
    early, late = slice(0, cut - size), slice(cut - size, cut)

    @pl.loop(0, count)
    def _(source):
        block = pl.ds(pl.multiple_of(shard_ref[source] * rows, rows), rows)
        pltpu.make_async_copy(
            query_all.at[source], query_slice.at[0, block, :], sems.at[0]
        ).start()
        pltpu.make_async_copy(
            output_all.at[source], output_slice.at[0, :, block], sems.at[1]
        ).start()

    prints = [
        pltpu.make_async_copy(
            query_prints.at[0, :, early], query_result.at[0, :, early], sems.at[2]
        ),
        pltpu.make_async_copy(
            output_prints.at[0, early, :], output_result.at[0, early, :], sems.at[3]
        ),
    ]
    for copy in prints:
        copy.start()
    query_last[...] = query_prints[0, :, late]
    output_last[...] = output_prints[0, late, :]

    @pl.loop(tp_count // 2, tp_count)
    def _(offset):
        for g in range(rep_count):
            source = g * tp_count + pair_index(tp, offset, tp_count)
            along = slice(g * rows, (g + 1) * rows)
            picked[:, along] = probes[shard_ref[source]]
            query_tile[along, :] = query_all[source, :, late]
            output_tile[:, along] = output_all[source, late, :]
        query_last[...] += jnp.dot(
            picked[...], query_tile[...], preferred_element_type=jnp.float32
        )
        output_last[...] += lax.dot_general(
            output_tile[...], picked[...], (((1,), (1,)), ((), ())),
            preferred_element_type=jnp.float32,
        )

    prints += [
        pltpu.make_async_copy(query_last, query_result.at[0, :, late], sems.at[4]),
        pltpu.make_async_copy(output_last, output_result.at[0, late, :], sems.at[5]),
    ]
    for copy in prints[2:]:
        copy.start()
    for k, everything in enumerate((query_all, output_all)):
        pltpu.make_async_copy(everything, everything, sems.at[k]).wait()
    for copy in prints:
        copy.wait()


def place(moved, shard_block):
    query_all, output_all, query_prints, output_prints, probes = moved
    count, rows, cut = query_all.shape
    kinds = probes.shape[1]
    size = cut // 4
    depth = lax.axis_size("rep") * rows
    inside = pl.BlockSpec(memory_space=pltpu.VMEM)
    return pl.pallas_call(
        place_kernel,
        out_shape=(
            jax.ShapeDtypeStruct((1, count * rows, cut), jnp.bfloat16),
            jax.ShapeDtypeStruct((1, cut, count * rows), jnp.bfloat16),
            jax.ShapeDtypeStruct(query_prints.shape, jnp.float32),
            jax.ShapeDtypeStruct(output_prints.shape, jnp.float32),
        ),
        in_specs=[pl.BlockSpec(memory_space=pltpu.SMEM)] + [inside] * 5,
        out_specs=[pl.BlockSpec(memory_space=pl.ANY)] * 4,
        scratch_shapes=[
            pltpu.VMEM((kinds, size), jnp.float32),
            pltpu.VMEM((size, kinds), jnp.float32),
            pltpu.VMEM((kinds, depth), jnp.bfloat16),
            pltpu.VMEM((depth, size), jnp.bfloat16),
            pltpu.VMEM((size, depth), jnp.bfloat16),
            pltpu.SemaphoreType.DMA((6,)),
        ],
        compiler_params=pltpu.CompilerParams(vmem_limit_bytes=VMEM_LIMIT),
    )(shard_block, *(pltpu.with_memory_space_constraint(x, pltpu.VMEM) for x in moved))


def per_device(trainer_query, trainer_output, probes, shard_block, slice_owner):
    tp_count = lax.axis_size("tp")
    rep_count = lax.axis_size("rep")
    count = tp_count * rep_count
    rows, width = trainer_query.shape[1:]
    cut = width // tp_count
    model = rows * count
    if rep_count == 4 and tp_count == 8 and rows % 128 == 0 and cut == 4 * rows:
        moved = stream(
            trainer_query, trainer_output, probes, shard_block, slice_owner, rep_count
        )
        return place(moved, shard_block)
    positions = jnp.arange(count, dtype=jnp.int32)
    held = shard_block[None, :] == positions[:, None]
    inverse = jnp.sum(jnp.where(held, positions[None, :], 0), axis=1, dtype=jnp.int32)
    query_blocks, output_blocks = pack(trainer_query, trainer_output, slice_owner)
    multiply = rows % 128 == 0
    moved = move(query_blocks, output_blocks, probes, shard_block, rep_count, multiply)
    if multiply:
        query_all, output_all, query_prints, output_prints = moved
        query_slice, output_slice = order(query_all, output_all, inverse)
        return query_slice, output_slice, query_prints, output_prints
    query_all, output_all = moved
    query_slice, query_prints = finish(
        query_kernel, query_all, probes, inverse,
        (1, model, cut), (1, probes.shape[0], cut), 0,
    )
    output_slice, output_prints = finish(
        output_kernel, output_all, probes, inverse,
        (1, cut, model), (1, cut, probes.shape[0]), 1,
    )
    return query_slice, output_slice, query_prints, output_prints


def solution(mesh):
    placed = (P(("rep", "tp"), None, None), P(("rep", "tp"), None, None), P(), P(), P())
    return jax.shard_map(
        per_device,
        mesh=mesh,
        in_specs=placed,
        out_specs=(
            P("tp", None, None),
            P("tp", None, None),
            P("tp", None, None),
            P("tp", None, None),
        ),
        check_vma=False,
    )
```
